32 devices in a mesh: node: 2 (over y), space: 16 (over z, x, core).
Axes of the slice: x: 2, y: 2, z: 4, core: 2. Of those that a mesh axis runs over, the one named last changes fastest.
Arguments:
- u_start: float32 [128, 256, 128], P('space'), may hold values from 0 to 1
- v_start: float32 [128, 256, 128], P('space'), may hold values from 0 to 2
- labels: int32 [128, 256, 128], P('space'), may hold values from 0 to 2
- u_guess: float32 [4, 128, 256, 128], P('node', 'space'), may hold values from 0 to 1
- v_guess: float32 [4, 128, 256, 128], P('node', 'space'), may hold values from 0 to 2
Outputs:
- u_nodes: float32 [4, 128, 256, 128], P('node', 'space')
- v_nodes: float32 [4, 128, 256, 128], P('node', 'space')
The draws below stay inside these ranges and needn't reach their ends.
Inputs may be any that keep to these rules, and one draw needn't show every extreme that they name: `labels`: 0 marks healthy, 1 fibrous and 2 scar tissue.
All inputs are finite; a program needn't handle non-finite values.
Results may differ from the reference program's by a relative error of at most 0.0001.
Values sent between devices are 32-bit elements; how exact they have to be, the bound alone decides.
No kernel may reach another device: no remote copies, remote signals or barrier semaphores. Data moves between devices by JAX's collectives and lax.ppermute only.
A program may use at most 192 MiB of HBM per device.

```python
import jax
import jax.numpy as jnp
from jax import lax

NY = 256
NZ = 128
NODES = 4
SWEEPS = 2
NX = 128


def set_ends(result, rng, smallest, largest):
    longest = result.shape.index(max(result.shape))
    spots = []
    for shift in (0, 1):
        where = [jax.random.randint(jax.random.fold_in(rng, axis), (), 0, length) for axis, length in enumerate(result.shape)]
        where[longest] = (where[longest] + shift) % result.shape[longest]
        spots.append(tuple(where))
    return result.at[spots[0]].set(smallest).at[spots[1]].set(largest)


def levels(own_key, shape, split, smallest, top_value):
    def one(dim, shards_of):
        heights = jax.random.uniform(jax.random.fold_in(jax.random.fold_in(own_key, 6), dim), (shards_of,), jnp.float32, smallest / len(split), top_value / len(split))
        return jnp.repeat(jnp.exp(heights), shape[dim] // shards_of).reshape((-1,) + (1,) * (len(shape) - dim - 1))

    gain = one(*split[0])
    for cut in split[1:]:
        gain = gain * one(*cut)
    return gain


def setup_inputs(seed: int = 0) -> dict:
    seeds = jax.random.split(jax.random.key(seed), 6)
    return {
        "u_start": jnp.clip(1.0 * jax.random.uniform(seeds[0], (NX, NY, NZ), jnp.float32) ** levels(seeds[0], (NX, NY, NZ), ((0, 16),), -0.2, 0.2), 0.0, 1.0),
        "v_start": jnp.clip(2.0 * jax.random.uniform(seeds[1], (NX, NY, NZ), jnp.float32) ** levels(seeds[1], (NX, NY, NZ), ((0, 16),), -0.2, 0.2), 0.0, 2.0),
        "labels": set_ends(jax.random.randint(seeds[2], (NX, NY, NZ), 0, 3), jax.random.fold_in(seeds[2], 1), 0, 2).astype(jnp.int32),
        "u_guess": jnp.clip(1.0 * jax.random.uniform(seeds[3], (NODES, NX, NY, NZ), jnp.float32) ** levels(seeds[3], (NODES, NX, NY, NZ), ((0, 2), (1, 16)), -0.2, 0.2), 0.0, 1.0),
        "v_guess": jnp.clip(2.0 * jax.random.uniform(seeds[4], (NODES, NX, NY, NZ), jnp.float32) ** levels(seeds[4], (NODES, NX, NY, NZ), ((0, 2), (1, 16)), -0.2, 0.2), 0.0, 2.0),
    }


radau_points = (0.08858795951270395, 0.4094668644407347, 0.7876594617608471, 1.0)
time_step = 0.16
onset_level = 0.15
ionic_gain = 8.0
recovery_base = 0.002
recovery_slope = 0.2
recovery_offset = 0.3
conductances = (1.0, 0.35, 0.05)
excitability = (1.0, 0.6, 0.0)


def weight_table():
    table = []
    for target in range(4):
        entries = []
        for column in range(4):
            coeffs = [1.0]
            for other in range(4):
                if other != column:
                    factor = 1.0 / (radau_points[column] - radau_points[other])
                    raised = [0.0] + coeffs
                    lowered = coeffs + [0.0]
                    coeffs = [factor * (raised[place] - radau_points[other] * lowered[place]) for place in range(len(raised))]
            integral = 0.0
            for place in range(len(coeffs)):
                integral = integral + coeffs[place] * radau_points[target] ** (place + 1) / (place + 1)
            entries.append(time_step * integral)
        table.append(entries)
    return table


def label_values(labels, values):
    return jnp.where(labels == 0, jnp.float32(values[0]),
                     jnp.where(labels == 1, jnp.float32(values[1]), jnp.float32(values[2])))


def neighbours(field):
    padded = jnp.pad(field, 1)
    return (padded[2:, 1:-1, 1:-1], padded[:-2, 1:-1, 1:-1],
            padded[1:-1, 2:, 1:-1], padded[1:-1, :-2, 1:-1],
            padded[1:-1, 1:-1, 2:], padded[1:-1, 1:-1, :-2])


def rates(u_field, v_field, conduct, excite):
    conduct_sides = neighbours(conduct)
    voltage_sides = neighbours(u_field)
    spread = jnp.zeros_like(u_field)
    for conduct_side, voltage_side in zip(conduct_sides, voltage_sides):
        facing = 2.0 * conduct * conduct_side / (conduct + conduct_side)
        spread = spread + facing * (voltage_side - u_field)
    ionic = ionic_gain * u_field * (u_field - onset_level) * (1.0 - u_field) - u_field * v_field
    rate_u = spread + excite * ionic
    recovery = recovery_base + recovery_slope * v_field / jnp.maximum(u_field + recovery_offset, recovery_offset)
    rate_v = recovery * (-v_field - ionic_gain * u_field * (u_field - onset_level - 1.0))
    return rate_u, rate_v


def reference(u_start, v_start, labels, u_guess, v_guess):
    conduct = label_values(labels, conductances)
    excite = label_values(labels, excitability)
    weights = jnp.asarray(weight_table(), jnp.float32)
    u_nodes, v_nodes = u_guess, v_guess
    for sweep_index in range(SWEEPS):
        rate_u, rate_v = lax.map(lambda node_pair: rates(node_pair[0], node_pair[1], conduct, excite), (u_nodes, v_nodes))
        u_nodes = u_start[None] + jnp.einsum("ij,jabc->iabc", weights, rate_u, precision=lax.Precision.HIGHEST)
        v_nodes = v_start[None] + jnp.einsum("ij,jabc->iabc", weights, rate_v, precision=lax.Precision.HIGHEST)
    return u_nodes, v_nodes
```

```python
import jax
import jax.numpy as jnp
from jax import lax
from jax.experimental import pallas as pl
from jax.experimental.pallas import tpu as pltpu
from jax.sharding import PartitionSpec as P

SWEEPS = 2


radau_points = (0.08858795951270395, 0.4094668644407347, 0.7876594617608471, 1.0)
time_step = 0.16
onset_level = 0.15
ionic_gain = 8.0
recovery_base = 0.002
recovery_slope = 0.2
recovery_offset = 0.3
conductances = (1.0, 0.35, 0.05)
excitability = (1.0, 0.6, 0.0)


def weight_table():
    table = []
    for target in range(4):
        entries = []
        for column in range(4):
            coeffs = [1.0]
            for other in range(4):
                if other != column:
                    factor = 1.0 / (radau_points[column] - radau_points[other])
                    raised = [0.0] + coeffs
                    lowered = coeffs + [0.0]
                    coeffs = [
                        factor * (raised[place] - radau_points[other] * lowered[place])
                        for place in range(len(raised))
                    ]
            integral = 0.0
            for place in range(len(coeffs)):
                integral = integral + coeffs[place] * radau_points[target] ** (place + 1) / (
                    place + 1
                )
            entries.append(time_step * integral)
        table.append(entries)
    return table


def label_values(labels, values):
    return jnp.where(
        labels == 0,
        jnp.float32(values[0]),
        jnp.where(labels == 1, jnp.float32(values[1]), jnp.float32(values[2])),
    )

STRIP = 16
PAD = 8


def face(center, beside):
    return 2.0 * center * beside / (center + beside)


def sweep_call(first, second, total, weights, sources, results):
    rows, lanes = sources["us", 0][0].shape[-2:]
    own = total // 2
    arrays, place, order = [], {}, []

    def need(key):
        if key in place or (key[0] in ("u1", "v1") and key[-1] in first):
            return
        array, index = sources[key]
        for spot, known in enumerate(arrays):
            if known is array:
                break
        else:
            spot = len(arrays)
            arrays.append(array)
        place[key] = (spot, index)
        order.append(key)

    def needs(names, plane):
        need(("fx", plane))
        need(("fx", plane + 1))
        for name in ("fy", "fz", "e", "us", "vs"):
            need((name, plane))
        for node in range(total):
            for offset in (0, -1, 1):
                need((names[0], node, plane + offset))
            need((names[1], node, plane))

    for plane in first:
        needs(("u", "v"), plane)
    for plane in second:
        needs(("u1", "v1"), plane)
    fetched = len(order)
    slots = {key: spot for spot, key in enumerate(order)}
    made = [(name, node, plane) for plane in first for name in ("u1", "v1") for node in range(total)]
    ended = [(name, node, plane) for plane in second for name in ("u2", "v2") for node in range(own)]
    for key in made + ended:
        slots[key] = len(slots)
    written = len(made) + len(ended)
    outs = []
    if first:
        shape = (total, len(first), rows, lanes)
        outs += [jax.ShapeDtypeStruct(shape, jnp.float32)] * 2
    if second:
        shape = (own, len_planes(sources), rows, lanes)
        outs += [jax.ShapeDtypeStruct(shape, jnp.float32)] * 2
    operands = [weights] + arrays
    aliases = {}
    if second and results is not None:
        aliases = {len(operands): len(outs) - 2, len(operands) + 1: len(outs) - 1}
        operands = operands + list(results)
    inputs = len(operands)

    def kernel(*refs):
        weight_ref, array_refs = refs[0], refs[1:1 + len(arrays)]
        out_refs = refs[inputs:inputs + len(outs)]
        buf, arrive, leave = refs[inputs + len(outs):]
        copies = {}
        for spot, key in enumerate(order):
            which, index = place[key]
            copies[key] = pltpu.make_async_copy(
                array_refs[which].at[index], buf.at[slots[key], pl.ds(PAD, rows)], arrive.at[spot])
            copies[key].start()
        blank = jnp.zeros((PAD, lanes), jnp.float32)
        for key, spot in slots.items():
            if key[0] in ("u", "u1", "fy"):
                buf[spot, pl.ds(0, PAD), :] = blank
                buf[spot, pl.ds(PAD + rows, PAD), :] = blank
        weight = [[weight_ref[m, j] for j in range(total)] for m in range(total)]
        waited = set()
        sends = []

        def ready(key):
            if key in copies and key not in waited:
                waited.add(key)
                copies[key].wait()

        def sweep(names, outs_named, plane, targets):
            for key in ([("fx", plane), ("fx", plane + 1)]
                        + [(name, plane) for name in ("fy", "fz", "e", "us", "vs")]
                        + [(names[0], node, plane + o) for node in range(total) for o in (0, -1, 1)]
                        + [(names[1], node, plane) for node in range(total)]):
                ready(key)

            def strip(step, carry):
                base = pl.multiple_of(step * STRIP, STRIP) + PAD

                def at(key, offset=0):
                    return buf[slots[key], pl.ds(base + offset, STRIP), :]

                before, after = at(("fx", plane)), at(("fx", plane + 1))
                above, below = at(("fy", plane)), at(("fy", plane), -1)
                right = at(("fz", plane))
                left = pltpu.roll(right, 1, 1)
                around = (after + before) + (above + below) + (right + left)
                excite = at(("e", plane))
                sum_u = [at(("us", plane)) for _ in range(targets)]
                sum_v = [at(("vs", plane)) for _ in range(targets)]
                for node in range(total):
                    u = at((names[0], node, plane))
                    v = at((names[1], node, plane))
                    spread = (after * at((names[0], node, plane + 1))
                              + before * at((names[0], node, plane - 1))
                              + (above * at((names[0], node, plane), 1)
                                 + below * at((names[0], node, plane), -1))
                              + (right * pltpu.roll(u, lanes - 1, 1) + left * pltpu.roll(u, 1, 1))
                              - around * u)
                    gain = ionic_gain * u
                    ionic = gain * (u - onset_level) * (1.0 - u) - u * v
                    rate_u = spread + excite * ionic
                    recovery = recovery_base + recovery_slope * v / jnp.maximum(
                        u + recovery_offset, recovery_offset)
                    rate_v = recovery * (-v - gain * (u - onset_level - 1.0))
                    for m in range(targets):
                        sum_u[m] = sum_u[m] + weight[m][node] * rate_u
                        sum_v[m] = sum_v[m] + weight[m][node] * rate_v
                for m in range(targets):
                    buf[slots[outs_named[0], m, plane], pl.ds(base, STRIP), :] = sum_u[m]
                    buf[slots[outs_named[1], m, plane], pl.ds(base, STRIP), :] = sum_v[m]
                return carry

            lax.fori_loop(0, rows // STRIP, strip, 0)

        def send(key, target):
            copy = pltpu.make_async_copy(
                buf.at[slots[key], pl.ds(PAD, rows)], target, leave.at[len(sends)])
            copy.start()
            sends.append(copy)

        for spot, plane in enumerate(first):
            sweep(("u", "v"), ("u1", "v1"), plane, total)
            for node in range(total):
                send(("u1", node, plane), out_refs[0].at[node, spot])
                send(("v1", node, plane), out_refs[1].at[node, spot])
        for plane in second:
            sweep(("u1", "v1"), ("u2", "v2"), plane, own)
            for node in range(own):
                send(("u2", node, plane), out_refs[-2].at[node, plane])
                send(("v2", node, plane), out_refs[-1].at[node, plane])
        for copy in sends:
            copy.wait()

    space = pl.BlockSpec(memory_space=pl.ANY)
    size = len(slots) * (rows + 2 * PAD) * lanes * 4 + (4 << 20)
    work = (len(first) + len(second)) * total * rows * lanes * 60
    result = pl.pallas_call(
        kernel,
        out_shape=tuple(outs),
        in_specs=[pl.BlockSpec(memory_space=pltpu.SMEM)] + [space] * (inputs - 1),
        out_specs=tuple([space] * len(outs)),
        scratch_shapes=[
            pltpu.VMEM((len(slots), rows + 2 * PAD, lanes), jnp.float32),
            pltpu.SemaphoreType.DMA((fetched,)),
            pltpu.SemaphoreType.DMA((written,)),
        ],
        input_output_aliases=aliases,
        compiler_params=pltpu.CompilerParams(vmem_limit_bytes=size),
        cost_estimate=pl.CostEstimate(flops=work, transcendentals=0,
                                      bytes_accessed=(fetched + written) * rows * lanes * 4),
    )(*operands)
    if first:
        for spot, plane in enumerate(first):
            for node in range(total):
                sources["u1", node, plane] = (result[0], (node, spot))
                sources["v1", node, plane] = (result[1], (node, spot))
    return result


def len_planes(sources):
    return sources["us", 0][0].shape[0]


def take(field, planes, dim=1):
    runs, start = [], 0
    for stop in range(1, len(planes) + 1):
        if stop == len(planes) or planes[stop] != planes[stop - 1] + 1:
            runs.append(lax.slice_in_dim(field, planes[start], planes[stop - 1] + 1, axis=dim))
            start = stop
    return runs[0] if len(runs) == 1 else jnp.concatenate(runs, axis=dim)


def on_device(u_start, v_start, labels, u_guess, v_guess):
    own, planes = u_guess.shape[:2]
    count = lax.axis_size("node")
    total = own * count
    reach = lax.axis_size("space")
    swap = [(i, (i + 1) % count) for i in range(count)]
    forward = [(i, i + 1) for i in range(reach - 1)]
    backward = [(i + 1, i) for i in range(reach - 1)]
    middle = planes // 2
    edges, last, late = [0, planes - 1], [middle], [middle - 1]
    inner = [p for p in range(1, planes - 1) if p not in last + late]

    def across(field, chunk):
        return lax.ppermute(take(field, chunk), "node", swap)

    chunks_u = [edges, list(range(1, planes - 1))]
    chunks_v = [edges, inner, late, last]
    others_u = [across(u_guess, chunk) for chunk in chunks_u]
    others_v = [across(v_guess, chunk) for chunk in chunks_v]

    conduct = label_values(labels, conductances)
    excite = label_values(labels, excitability)
    low = lax.ppermute(jnp.concatenate([u_guess[:, -1], conduct[-1:]]), "space", forward)
    high = lax.ppermute(jnp.concatenate([u_guess[:, 0], conduct[:1]]), "space", backward)
    low_far = lax.ppermute(others_u[0][:, 1], "space", forward)
    high_far = lax.ppermute(others_u[0][:, 0], "space", backward)

    extended = jnp.concatenate([low[own:], conduct, high[own:]])
    face_x = face(extended[1:-1], extended[:-2])
    face_x = jnp.concatenate([face_x, face(conduct[-1:], extended[-1:])])
    face_y = jnp.pad(face(conduct[:, :-1], conduct[:, 1:]), ((0, 0), (0, 1), (0, 0)))
    face_z = jnp.pad(face(conduct[:, :, :-1], conduct[:, :, 1:]), ((0, 0), (0, 0), (0, 1)))

    turned = (jnp.arange(total) + lax.axis_index("node") * own) % total
    weights = jnp.asarray(weight_table(), jnp.float32)[turned][:, turned]

    sources = {}
    for plane in range(planes + 1):
        sources["fx", plane] = (face_x, (plane,))
    for plane in range(planes):
        for name, array in (("fy", face_y), ("fz", face_z), ("e", excite), ("us", u_start), ("vs", v_start)):
            sources[name, plane] = (array, (plane,))
        for node in range(own):
            sources["u", node, plane] = (u_guess, (node, plane))
            sources["v", node, plane] = (v_guess, (node, plane))
    for name, chunks, others in (("u", chunks_u, others_u), ("v", chunks_v, others_v)):
        for chunk, array in zip(chunks, others):
            for spot, plane in enumerate(chunk):
                for node in range(own):
                    sources[name, own + node, plane] = (array, (node, spot))
    for node in range(own):
        sources["u", node, -1] = (low, (node,))
        sources["u", node, planes] = (high, (node,))
        sources["u", own + node, -1] = (low_far, (node,))
        sources["u", own + node, planes] = (high_far, (node,))

    first_u, first_v = sweep_call(edges, [], total, weights, sources, None)
    low_next = lax.ppermute(first_u[:, 1], "space", forward)
    high_next = lax.ppermute(first_u[:, 0], "space", backward)
    for node in range(total):
        sources["u1", node, -1] = (low_next, (node,))
        sources["u1", node, planes] = (high_next, (node,))
    done, closed, results = set(edges), set(), None
    for chunk in chunks_v[1:]:
        done |= set(chunk)
        second = [p for p in range(planes) if p not in closed
                  and {p - 1, p, p + 1} & set(range(planes)) <= done]
        closed |= set(second)
        results = sweep_call(chunk, second, total, weights, sources, results)[2:]
    return tuple(results)


def solution(mesh):
    return jax.shard_map(
        on_device,
        mesh=mesh,
        in_specs=(
            P("space", None, None),
            P("space", None, None),
            P("space", None, None),
            P("node", "space", None, None),
            P("node", "space", None, None),
        ),
        out_specs=(P("node", "space", None, None), P("node", "space", None, None)),
        check_vma=False,
    )
```

```python
import jax
import jax.numpy as jnp
from jax import lax
from jax.experimental import pallas as pl
from jax.experimental.pallas import tpu as pltpu
from jax.sharding import PartitionSpec as P


radau_points = (0.08858795951270395, 0.4094668644407347, 0.7876594617608471, 1.0)
time_step = 0.16
onset_level = 0.15
ionic_gain = 8.0
recovery_base = 0.002
recovery_slope = 0.2
recovery_offset = 0.3
conductances = (1.0, 0.35, 0.05)
excitability = (1.0, 0.6, 0.0)


def weight_table():
    table = []
    for target in range(4):
        entries = []
        for column in range(4):
            coeffs = [1.0]
            for other in range(4):
                if other != column:
                    factor = 1.0 / (radau_points[column] - radau_points[other])
                    raised = [0.0] + coeffs
                    lowered = coeffs + [0.0]
                    coeffs = [
                        factor * (raised[place] - radau_points[other] * lowered[place])
                        for place in range(len(raised))
                    ]
            integral = 0.0
            for place in range(len(coeffs)):
                integral = integral + coeffs[place] * radau_points[target] ** (place + 1) / (
                    place + 1
                )
            entries.append(time_step * integral)
        table.append(entries)
    return table


def label_values(labels, values):
    return jnp.where(
        labels == 0,
        jnp.float32(values[0]),
        jnp.where(labels == 1, jnp.float32(values[1]), jnp.float32(values[2])),
    )


STRIP = 16
LIMIT = None


def face(center, beside):
    return 2.0 * center * beside / (center + beside)


def sweep_call(first, second, total, weights, sources, results, keep=True):
    rows, lanes = sources["us", 0][0].shape[-2:]
    own = total // 2
    arrays, place = [], {}

    def need(key):
        if key in place or (key[0] in ("u1", "v1") and key[-1] in first):
            return
        array, index = sources[key]
        for spot, known in enumerate(arrays):
            if known is array:
                break
        else:
            spot = len(arrays)
            arrays.append(array)
        place[key] = (spot, index)

    def needs(names, plane):
        need(("fx", plane))
        need(("fx", plane + 1))
        for name in ("fy", "fz", "e", "us", "vs"):
            need((name, plane))
        for node in range(total):
            for offset in (0, -1, 1):
                need((names[0], node, plane + offset))
            need((names[1], node, plane))

    for plane in first:
        needs(("u", "v"), plane)
    for plane in second:
        needs(("u1", "v1"), plane)
    ended = [(name, node, plane) for plane in second for name in ("u2", "v2") for node in range(own)]
    if not keep:
        ended += [(name, node, plane) for plane in first for name in ("u1", "v1") for node in range(total)]
    slots = {key: spot for spot, key in enumerate(ended)}
    outs, kinds = [], []
    if first and keep:
        shape = (total, len(first), rows, lanes)
        outs += [jax.ShapeDtypeStruct(shape, jnp.float32)] * 2
        kinds += [pltpu.VMEM] * 2
    if second:
        shape = (own, len_planes(sources), rows, lanes)
        outs += [jax.ShapeDtypeStruct(shape, jnp.float32)] * 2
        kinds += [pl.ANY] * 2
    operands = [weights] + arrays
    aliases = {}
    if second and results is not None:
        aliases = {len(operands): len(outs) - 2, len(operands) + 1: len(outs) - 1}
        operands = operands + list(results)
    inputs = len(operands)

    def kernel(*refs):
        weight_ref, array_refs = refs[0], refs[1:1 + len(arrays)]
        out_refs = refs[inputs:inputs + len(outs)]
        weight = [[weight_ref[m, j] for j in range(total)] for m in range(total)]
        sends = []

        def view(key):
            if key in slots:
                return refs[-2], (slots[key],)
            if key in place:
                which, index = place[key]
                return array_refs[which], index
            return out_refs[0 if key[0] == "u1" else 1], (key[1], first.index(key[2]))

        def sweep(names, outs_named, plane, targets):
            def strip(base, top, bottom):
                def at(key):
                    ref, index = view(key)
                    return ref[index + (pl.ds(base, STRIP), slice(None))]

                def moved(key, offset):
                    ref, index = view(key)
                    if (top and offset < 0) or (bottom and offset > 0):
                        kept = ref[index + (pl.ds(base + max(offset, 0), STRIP - 1), slice(None))]
                        edge = ref[index + (pl.ds(base + (STRIP - 1 if bottom else 0), 1), slice(None))]
                        if key[0] == "fy":
                            edge = jnp.zeros_like(edge)
                        return jnp.concatenate([edge, kept] if offset < 0 else [kept, edge])
                    return ref[index + (pl.ds(base + offset, STRIP), slice(None))]

                before, after = at(("fx", plane)), at(("fx", plane + 1))
                above, below = at(("fy", plane)), moved(("fy", plane), -1)
                right = at(("fz", plane))
                left = pltpu.roll(right, 1, 1)
                around = (after + before) + (above + below) + (right + left)
                excite = at(("e", plane))
                sum_u = [at(("us", plane)) for _ in range(targets)]
                sum_v = [at(("vs", plane)) for _ in range(targets)]
                for node in range(total):
                    u = at((names[0], node, plane))
                    v = at((names[1], node, plane))
                    spread = (after * at((names[0], node, plane + 1))
                              + before * at((names[0], node, plane - 1))
                              + (above * moved((names[0], node, plane), 1)
                                 + below * moved((names[0], node, plane), -1))
                              + (right * pltpu.roll(u, lanes - 1, 1) + left * pltpu.roll(u, 1, 1))
                              - around * u)
                    gain = ionic_gain * u
                    ionic = gain * (u - onset_level) * (1.0 - u) - u * v
                    rate_u = spread + excite * ionic
                    recovery = recovery_base + recovery_slope * v / jnp.maximum(
                        u + recovery_offset, recovery_offset)
                    rate_v = recovery * (-v - gain * (u - onset_level - 1.0))
                    for m in range(targets):
                        sum_u[m] = sum_u[m] + weight[m][node] * rate_u
                        sum_v[m] = sum_v[m] + weight[m][node] * rate_v
                for m in range(targets):
                    for name, value in zip(outs_named, (sum_u[m], sum_v[m])):
                        ref, index = view((name, m, plane))
                        ref[index + (pl.ds(base, STRIP), slice(None))] = value

            def inside(step, carry):
                strip(pl.multiple_of(step * STRIP, STRIP), False, False)
                return carry

            strip(0, True, False)
            lax.fori_loop(1, rows // STRIP - 1, inside, 0)
            strip(rows - STRIP, False, True)

        def send(key, target):
            copy = pltpu.make_async_copy(refs[-2].at[slots[key]], target, refs[-1].at[len(sends)])
            copy.start()
            sends.append(copy)

        for plane in first:
            sweep(("u", "v"), ("u1", "v1"), plane, total)
        for plane in second:
            sweep(("u1", "v1"), ("u2", "v2"), plane, own)
            for node in range(own):
                send(("u2", node, plane), out_refs[-2].at[node, plane])
                send(("v2", node, plane), out_refs[-1].at[node, plane])
        for copy in sends:
            copy.wait()

    spec = lambda kind: pl.BlockSpec(memory_space=kind)
    size = len(slots) * rows * lanes * 4 + (4 << 20)
    work = (len(first) + len(second)) * total * rows * lanes * 60
    result = pl.pallas_call(
        kernel,
        out_shape=tuple(outs),
        in_specs=[spec(pltpu.SMEM)] + [spec(pltpu.VMEM)] * len(arrays)
        + [spec(pl.ANY)] * (inputs - 1 - len(arrays)),
        out_specs=tuple(spec(kind) for kind in kinds),
        scratch_shapes=[
            pltpu.VMEM((len(slots), rows, lanes), jnp.float32),
            pltpu.SemaphoreType.DMA((len(slots),)),
        ] if slots else [],
        input_output_aliases=aliases,
        compiler_params=pltpu.CompilerParams(vmem_limit_bytes=LIMIT or size),
        cost_estimate=pl.CostEstimate(flops=work, transcendentals=0,
                                      bytes_accessed=len(arrays) * rows * lanes * 4),
    )(*operands)
    if first and keep:
        for spot, plane in enumerate(first):
            for node in range(total):
                sources["u1", node, plane] = (result[0], (node, spot))
                sources["v1", node, plane] = (result[1], (node, spot))
    return result


def len_planes(sources):
    return sources["us", 0][0].shape[0]


def take(field, planes, dim=1):
    runs, start = [], 0
    for stop in range(1, len(planes) + 1):
        if stop == len(planes) or planes[stop] != planes[stop - 1] + 1:
            runs.append(lax.slice_in_dim(field, planes[start], planes[stop - 1] + 1, axis=dim))
            start = stop
    return runs[0] if len(runs) == 1 else jnp.concatenate(runs, axis=dim)


def step(u_start, v_start, labels, u_guess, v_guess):
    own, planes = u_guess.shape[:2]
    count = lax.axis_size("node")
    total = own * count
    reach = lax.axis_size("space")
    swap = [(i, (i + 1) % count) for i in range(count)]
    forward = [(i, i + 1) for i in range(reach - 1)]
    backward = [(i + 1, i) for i in range(reach - 1)]
    middle = planes // 2
    edges, last, late = [0, planes - 1], [middle], [middle - 1]
    inner = [p for p in range(1, planes - 1) if p not in last + late]

    def across(field, chunk):
        return lax.ppermute(take(field, chunk), "node", swap)

    chunks_u = [list(range(planes))]
    chunks_v = [edges, inner, late, last]
    others_u = [across(u_guess, chunk) for chunk in chunks_u]
    others_v = [across(v_guess, chunk) for chunk in chunks_v]

    conduct = label_values(labels, conductances)
    excite = label_values(labels, excitability)
    low = lax.ppermute(jnp.concatenate([u_guess[:, -1], conduct[-1:]]), "space", forward)
    high = lax.ppermute(jnp.concatenate([u_guess[:, 0], conduct[:1]]), "space", backward)
    low_far = lax.ppermute(others_u[0][:, -1], "space", forward)
    high_far = lax.ppermute(others_u[0][:, 0], "space", backward)

    extended = jnp.concatenate([low[own:], conduct, high[own:]])
    face_x = face(extended[1:-1], extended[:-2])
    face_x = jnp.concatenate([face_x, face(conduct[-1:], extended[-1:])])
    face_y = jnp.pad(face(conduct[:, :-1], conduct[:, 1:]), ((0, 0), (0, 1), (0, 0)))
    face_z = jnp.pad(face(conduct[:, :, :-1], conduct[:, :, 1:]), ((0, 0), (0, 0), (0, 1)))

    turned = (jnp.arange(total) + lax.axis_index("node") * own) % total
    weights = jnp.asarray(weight_table(), jnp.float32)[turned][:, turned]

    sources = {}
    for plane in range(planes + 1):
        sources["fx", plane] = (face_x, (plane,))
    for plane in range(planes):
        for name, array in (("fy", face_y), ("fz", face_z), ("e", excite), ("us", u_start), ("vs", v_start)):
            sources[name, plane] = (array, (plane,))
        for node in range(own):
            sources["u", node, plane] = (u_guess, (node, plane))
            sources["v", node, plane] = (v_guess, (node, plane))
    for name, chunks, others in (("u", chunks_u, others_u), ("v", chunks_v, others_v)):
        for chunk, array in zip(chunks, others):
            for spot, plane in enumerate(chunk):
                for node in range(own):
                    sources[name, own + node, plane] = (array, (node, spot))
    for node in range(own):
        sources["u", node, -1] = (low, (node,))
        sources["u", node, planes] = (high, (node,))
        sources["u", own + node, -1] = (low_far, (node,))
        sources["u", own + node, planes] = (high_far, (node,))

    first_u, _ = sweep_call(edges, [], total, weights, sources, None)
    low_next = lax.ppermute(first_u[:, 1], "space", forward)
    high_next = lax.ppermute(first_u[:, 0], "space", backward)
    for node in range(total):
        sources["u1", node, -1] = (low_next, (node,))
        sources["u1", node, planes] = (high_next, (node,))
    near = [p for p in range(middle - 2, middle + 2) if 0 <= p < planes]
    centre = take(others_u[0], near)
    for spot, plane in enumerate(near):
        for node in range(own):
            sources["u", own + node, plane, "near"] = (centre, (node, spot))
    done, closed, results = set(edges), set(), None
    for chunk in chunks_v[1:]:
        done |= set(chunk)
        second = [p for p in range(planes) if p not in closed
                  and {p - 1, p, p + 1} & set(range(planes)) <= done]
        closed |= set(second)
        if chunk is not inner:
            for plane in near:
                for node in range(own, total):
                    sources["u", node, plane] = sources["u", node, plane, "near"]
        results = sweep_call(chunk, second, total, weights, sources, results, chunk is not last)[-2:]
    return tuple(results)


def solution(mesh):
    return jax.shard_map(
        step,
        mesh=mesh,
        in_specs=(
            P("space", None, None),
            P("space", None, None),
            P("space", None, None),
            P("node", "space", None, None),
            P("node", "space", None, None),
        ),
        out_specs=(P("node", "space", None, None), P("node", "space", None, None)),
        check_vma=False,
    )
```
